128 devices in a mesh: row: 8 (over y, core), col: 16 (over x, z).
Axes of the slice: x: 4, y: 4, z: 4, core: 2. Of those that a mesh axis runs over, the one named last changes fastest.
Arguments:
- matrix_in: float32 [4, 4096, 2, 8192], P(None, 'row', None, 'col'), as said below
- panel_start: int32 [1], replicated, may hold values from 0 to 29
Outputs:
- matrix_out: float32 [4, 4096, 2, 8192], P(None, 'row', None, 'col')
The draws below stay inside these ranges and needn't reach their ends.
Inputs may be any that keep to these rules, and one draw needn't show every extreme that they name: matrix_in is symmetric and positive definite.
All inputs are finite; a program needn't handle non-finite values.
Results may differ from the reference program's by a relative error of at most 0.0001.
Values sent between devices are 32-bit elements.
A program may use at most 128 MiB of HBM per device.

```python
import jax
import jax.numpy as jnp
from jax import lax

ORDER = 16384
NB = 512
PANELS = 2
BLOCKS = 32
LOC_BR = 4
LOC_BC = 2


def draw_matrix_in(key, part):
    key_gen = jax.random.fold_in(key, 21)
    key_shift = jax.random.fold_in(key, 22)
    inner_count = max(2 * NB, ORDER // 16)
    generator = jax.random.truncated_normal(key_gen, -6.0, 6.0, (ORDER, inner_count), jnp.float32)
    shift = jax.random.uniform(key_shift, (ORDER,), jnp.float32, 0.4, 0.8)
    common = jnp.zeros((ORDER,), jnp.float32)
    scales = jnp.ones((ORDER,), jnp.float32)
    weight = 0.0
    gram = lax.dot_general(generator, generator, (((1,), (1,)), ((), ())), precision=lax.Precision.HIGHEST, preferred_element_type=jnp.float32)
    gram = gram * (1.0 / inner_count)
    gram = 0.5 * (gram + gram.T)
    matrix = gram + weight * common[:, None] * common[None, :] + jnp.diag(shift)
    matrix = scales[:, None] * matrix * scales[None, :]
    return matrix.reshape(LOC_BR, ORDER // LOC_BR, LOC_BC, ORDER // LOC_BC)


def setup_inputs(seed: int = 0) -> dict:
    arg_keys = jax.random.split(jax.random.key(seed), 3)
    matrix_in = draw_matrix_in(jax.random.fold_in(arg_keys[2], 71), 0)
    panel_start = jax.random.randint(arg_keys[1], (1,), 0, BLOCKS - 2).astype(jnp.int32)
    return dict(matrix_in=matrix_in, panel_start=panel_start)


def reference(matrix_in, panel_start):
    matrix = matrix_in.reshape(ORDER, ORDER)
    block_index = jnp.arange(ORDER, dtype=jnp.int32) // NB
    first_panel = panel_start[0].astype(jnp.int32)
    for panel_step in range(PANELS):
        panel = first_panel + panel_step
        offset = (panel * NB).astype(jnp.int32)
        zero_index = jnp.zeros((), jnp.int32)
        diag_block = lax.dynamic_slice(matrix, (offset, offset), (NB, NB))
        factor = jnp.linalg.cholesky(diag_block)
        column_strip = lax.dynamic_slice(matrix, (zero_index, offset), (ORDER, NB))
        solved = jax.scipy.linalg.solve_triangular(factor, column_strip.T, lower=True).T
        below_panel = (block_index > panel)[:, None]
        column = jnp.where(below_panel, solved, jnp.float32(0.0))
        product = lax.dot_general(column.astype(jnp.float32), column.astype(jnp.float32), (((1,), (1,)), ((), ())), precision=lax.Precision.HIGHEST, preferred_element_type=jnp.float32)
        matrix = matrix - product
        new_strip = jnp.where(below_panel, solved, column_strip)
        new_strip = lax.dynamic_update_slice(new_strip, factor, (offset, zero_index))
        matrix = lax.dynamic_update_slice(matrix, new_strip, (zero_index, offset))
    return matrix.reshape(matrix_in.shape)
```

```python
import functools

import jax
import jax.numpy as jnp
from jax import lax
from jax.experimental import pallas as pl
from jax.experimental.pallas import tpu as pltpu
from jax.sharding import PartitionSpec as P

MESH = pl.DeviceIdType.MESH
HI = lax.Precision.HIGHEST
NB = 512
TILE = 128
GR = TILE // 8


R = 32
CPB = 128 // R
YR = 256
NY = 2048 // YR


def comm_kernel(k, m_hbm, rp, cp, g, mbuf, ld_sem, cl_sem, gl_sem, pr_sem, ps_sem, yr_sem, ys_sem, yd_sem, yds_sem, gr_sem, gs_sem, gd_sem, gds_sem):
    r, c = lax.axis_index("row"), lax.axis_index("col")
    y, core = r // 2, r % 2
    x, z = c // 4, c % 4

    def at(xx, zz):
        return (r, lax.rem(xx + 4, 4) * 4 + lax.rem(zz + 4, 4))

    partner = (r + 1 - 2 * core, c)

    def ynb(sig):
        return (lax.rem(y + sig + 4, 4) * 2 + core, c)

    barrier = pltpu.get_barrier_semaphore()
    for nb in (at(x + 1, z), at(x - 1, z), at(x, z + 1), at(x, z - 1), ynb(1), ynb(-1), partner):
        pl.semaphore_signal(barrier, inc=1, device_id=nb, device_id_type=MESH)
    pl.semaphore_wait(barrier, 7)

    ks = (k, k + 1)
    own_c = [kk % 16 for kk in ks]
    own_j = [kk // 16 for kk in ks]
    own_r = [kk % 8 for kk in ks]
    own_i = [kk // 8 for kk in ks]
    nblk = [4 - i for i in own_i]
    is_c = [c == v for v in own_c]
    is_r = [r == v for v in own_r]

    def copy(src, dst, ssem, rsem, dev):
        return pltpu.make_async_remote_copy(src_ref=src, dst_ref=dst, send_sem=ssem, recv_sem=rsem, device_id=dev, device_id_type=MESH)

    info = []
    for p in range(2):
        rx, rz = own_c[p] // 4, own_c[p] % 4
        for t in range(4):
            sig = 1 if t % 2 == 0 else -1
            dx = lax.rem(sig * (x - rx) + 8, 4)
            dz = lax.rem(sig * (z - rz) + 8, 4)
            a, b = (dx, dz) if t < 2 else (dz, dx)
            depth = jnp.where(jnp.logical_and(a == 0, b != 0), 4 + b, a + b)
            nx, nz = at(x + sig, z), at(x, z + sig)
            n1, n2 = (nx, nz) if t < 2 else (nz, nx)
            s1 = jnp.logical_or(jnp.logical_and(b == 0, a < 3), jnp.logical_and(b != 0, a == 3))
            s2 = jnp.logical_and(a != 0, b < 3)
            root = jnp.logical_and(a == 0, b == 0)
            info.append((p, t, depth, n1, n2, s1, s2, root))

    def chunk(p, t, ch):
        i = own_i[p] + ch // CPB
        row = pl.multiple_of(t * 128 + lax.rem(ch, CPB) * R, R)
        return rp.at[p, i, pl.ds(row, R), :]

    def spread(p, i):
        pltpu.make_async_copy(m_hbm.at[pl.ds(i * 4096, 4096), :], mbuf.at[pl.ds(i * 4096, 4096), :], ld_sem.at[i]).wait()

        def group(q, _):
            for l in range(4):
                v = mbuf[pl.ds(i * 4096 + q * 512 + 2 * l + own_j[p], 64, stride=8), :]
                rp[p, i, pl.ds(pl.multiple_of(q * 64, 64), 64), l * 128 : l * 128 + 128] = v
            return 0

        lax.fori_loop(0, 8, group, 0)

    for p in range(2):
        slab = pltpu.make_async_copy(m_hbm.at[pl.ds(own_i[p] * 4096, 4096), :], cp.at[p], cl_sem.at[p])

        @pl.when(is_r[p])
        def _():
            slab.start()

    for p in range(2):
        @pl.when(is_c[p])
        def _():
            for i in range(own_i[p], 4):
                pltpu.make_async_copy(m_hbm.at[pl.ds(i * 4096, 4096), :], mbuf.at[pl.ds(i * 4096, 4096), :], ld_sem.at[i]).start()
            spread(p, own_i[p])

    def dist(p, sig):
        return lax.rem(sig * (y - own_r[p] // 2) + 8, 4)

    def ychunk(p, d, u):
        return cp.at[p, pl.ds(pl.multiple_of(d * 2048 + u * YR, YR), YR), :]

    def ysend(p, d, u):
        sl = ychunk(p, d, u)
        copy(sl, sl, ys_sem.at[p, d], yr_sem.at[p, d, u], ynb(1 - 2 * d)).start()

    def ydown(p, d, u):
        sl = ychunk(p, d, u)
        copy(sl, sl, yds_sem.at[p], yd_sem.at[p], partner).start()

    for p in range(2):
        @pl.when(is_r[p])
        def _():
            pltpu.make_async_copy(m_hbm.at[pl.ds(own_i[p] * 4096, 4096), :], cp.at[p], cl_sem.at[p]).wait()

    gl = ((0, 0, own_i[0]), (1, 0, own_i[1]), (1, 1, own_i[1]))

    def gchunk(gi, t, q):
        return g.at[gi, pl.ds(pl.multiple_of(t * 128 + q * R, R), R), :]

    def gsrc(gi, t, q):
        o, p, i = gl[gi]
        return rp.at[p, i, pl.ds(pl.multiple_of(t * 128 + q * R, R), R), :]

    def gsend(gi, t, q, src):
        o, p, i = gl[gi]
        d = t % 2
        dst = gchunk(gi, t, q)

        @pl.when(dist(o, 1 - 2 * d) < 3)
        def _():
            copy(src, dst, gs_sem.at[gi, d], gr_sem.at[gi, t, q], ynb(1 - 2 * d)).start()

        copy(src, dst, gds_sem.at[gi], gd_sem.at[gi], partner).start()

    steps = max(4 * max(nblk) // 4 * CPB + 8, (own_i[1] - own_i[0] + 1) * CPB + 12, NY + 4)

    def step(s, _):
        for p, t, depth, n1, n2, s1, s2, root in info:
            ch = s - depth
            live = jnp.logical_and(ch >= 0, ch < nblk[p] * CPB)

            @pl.when(live)
            def _():
                sl = chunk(p, t, ch)

                @pl.when(jnp.logical_not(root))
                def _():
                    copy(sl, sl, ps_sem.at[p, t, 0], pr_sem.at[p, t, ch], n1).wait_recv()

                @pl.when(s1)
                def _():
                    copy(sl, sl, ps_sem.at[p, t, 0], pr_sem.at[p, t, ch], n1).start()

                @pl.when(s2)
                def _():
                    copy(sl, sl, ps_sem.at[p, t, 1], pr_sem.at[p, t, ch], n2).start()

            for gi in range(3):
                o, gp, i = gl[gi]
                if gp == p:
                    q = ch - (i - own_i[p]) * CPB

                    @pl.when(jnp.logical_and(is_r[o], jnp.logical_and(q >= 0, q < CPB)))
                    def _():
                        gsend(gi, t, q, gsrc(gi, t, q))

        for p in range(2):
            for d in range(2):
                dy = dist(p, 1 - 2 * d)
                u = s - dy
                ok = jnp.logical_and(jnp.logical_and(u >= 0, u < NY), core == own_r[p] % 2)

                @pl.when(ok)
                def _():
                    sl = ychunk(p, d, u)

                    @pl.when(dy > 0)
                    def _():
                        copy(sl, sl, ys_sem.at[p, d], yr_sem.at[p, d, u], partner).wait_recv()

                    @pl.when(dy < 3)
                    def _():
                        ysend(p, d, u)

                    ydown(p, d, u)

        for p, t, depth, n1, n2, s1, s2, root in info:
            for gi in range(3):
                o, gp, i = gl[gi]
                if gp == p:
                    dy = dist(o, 1 - 2 * (t % 2))
                    q = s - depth - dy - 1 - (i - own_i[p]) * CPB
                    ok = jnp.logical_and(jnp.logical_and(q >= 0, q < CPB), jnp.logical_and(dy > 0, core == own_r[o] % 2))

                    @pl.when(ok)
                    def _():
                        sl = gchunk(gi, t, q)
                        copy(sl, sl, gs_sem.at[gi, t % 2], gr_sem.at[gi, t, q], partner).wait_recv()
                        gsend(gi, t, q, sl)

        for p in range(2):
            @pl.when(jnp.logical_and(is_c[p], jnp.logical_and(lax.rem(s, CPB) == 1, s // CPB < nblk[p] - 1)))
            def _():
                spread(p, own_i[p] + 1 + s // CPB)
        return 0

    lax.fori_loop(0, steps, step, 0)

    for gi in range(3):
        o, p, i = gl[gi]

        @pl.when(is_r[o])
        def _():
            own = pltpu.make_async_copy(rp.at[p, i], g.at[gi], gl_sem.at[gi])
            own.start()
            own.wait()

    for p in range(2):
        @pl.when(core != own_r[p] % 2)
        def _():
            copy(cp.at[p], cp.at[p], yds_sem.at[p], yd_sem.at[p], partner).wait_recv()

        @pl.when(core == own_r[p] % 2)
        def _():
            copy(cp.at[p], cp.at[p], yds_sem.at[p], yd_sem.at[p], partner).wait_send()

            for d in range(2):
                @pl.when(dist(p, 1 - 2 * d) < 3)
                def _():
                    half = cp.at[p, pl.ds(d * 2048, 2048), :]
                    copy(half, half, ys_sem.at[p, d], yd_sem.at[p], partner).wait_send()

    for gi in range(3):
        o, p, i = gl[gi]

        @pl.when(core != own_r[o] % 2)
        def _():
            copy(g.at[gi], g.at[gi], gds_sem.at[gi], gd_sem.at[gi], partner).wait_recv()

        @pl.when(core == own_r[o] % 2)
        def _():
            copy(g.at[gi], g.at[gi], gds_sem.at[gi], gd_sem.at[gi], partner).wait_send()

            for d in range(2):
                @pl.when(dist(o, 1 - 2 * d) < 3)
                def _():
                    half = g.at[gi, pl.ds(0, 256), :]
                    copy(half, half, gs_sem.at[gi, d], gd_sem.at[gi], partner).wait_send()

    for p, t, depth, n1, n2, s1, s2, root in info:
        part = rp.at[p, pl.ds(0, nblk[p]), pl.ds(0, 128), :]
        for w, s in ((0, s1), (1, s2)):
            @pl.when(s)
            def _():
                copy(part, part, ps_sem.at[p, t, w], pr_sem.at[p, t, 0], partner).wait_send()


def gather(k, m_flat):
    f = jnp.float32
    vm = pl.BlockSpec(memory_space=pltpu.VMEM)
    dma = pltpu.SemaphoreType.DMA
    return pl.pallas_call(
        functools.partial(comm_kernel, k),
        out_shape=[jax.ShapeDtypeStruct((2, 4, NB, NB), f), jax.ShapeDtypeStruct((2, 4096, 128), f), jax.ShapeDtypeStruct((3, NB, NB), f)],
        in_specs=[pl.BlockSpec(memory_space=pl.ANY)], out_specs=[vm] * 3,
        scratch_shapes=[pltpu.VMEM((16384, 128), f), dma((4,)), dma((2,)), dma((3,)),
                        dma((2, 4, 4 * CPB)), dma((2, 4, 2)), dma((2, 2, NY)), dma((2, 2)), dma((2,)), dma((2,)),
                        dma((3, 4, CPB)), dma((3, 2)), dma((3,)), dma((3,))],
        compiler_params=pltpu.CompilerParams(collective_id=k, has_side_effects=True, vmem_limit_bytes=40 * 2**20),
        name="gather",
    )(m_flat)


def rep(v, i):
    return jnp.broadcast_to(v[i : i + 1, :], v.shape)


def lane(v, l):
    return jnp.broadcast_to(v[:, l : l + 1], v.shape)


def tile_factor(t_ref, v_ref):
    sub = lax.broadcasted_iota(jnp.int32, (8, TILE), 0)
    lan = lax.broadcasted_iota(jnp.int32, (8, TILE), 1)
    for g in range(GR):
        v_ref[8 * g : 8 * g + 8, :] = jnp.where(lan == sub + 8 * g, 1.0, 0.0).astype(jnp.float32)
    for g in range(GR):
        rows = slice(8 * g, 8 * g + 8)
        t = t_ref[rows, :]
        v = v_ref[rows, :]
        e = [lane(t, 8 * g + c) for c in range(8)]
        s, u = [], {}
        for j in range(8):
            sj = lax.rsqrt(rep(e[j], j))
            col = e[j] * sj
            s.append(sj)
            for c in range(j + 1, 8):
                u[j, c] = rep(col, c)
                e[c] = e[c] - col * u[j, c]
            colm = jnp.where(sub > j, col, 0.0)
            rt = rep(t, j) * sj
            rv = rep(v, j) * sj
            t = jnp.where(sub == j, rt, t - colm * rt)
            v = jnp.where(sub == j, rv, v - colm * rv)
        t_ref[rows, :] = t
        v_ref[rows, :] = v
        rts = [rep(t, c) for c in range(8)]
        rvs = [rep(v, c) for c in range(8)]
        for h in range(g + 1, GR):
            hr = slice(8 * h, 8 * h + 8)
            th = t_ref[hr, :]
            vh = v_ref[hr, :]
            f = [lane(th, 8 * g + c) for c in range(8)]
            for j in range(8):
                f[j] = f[j] * s[j]
                for c in range(j + 1, 8):
                    f[c] = f[c] - f[j] * u[j, c]
                th = th - f[j] * rts[j]
                vh = vh - f[j] * rvs[j]
            t_ref[hr, :] = th
            v_ref[hr, :] = vh


def factor_block(ab, t_ref, v_ref):
    def step(t, _):
        rows = pl.ds(pl.multiple_of(t * TILE, TILE), TILE)
        t_ref[...] = ab[rows, rows]
        tile_factor(t_ref, v_ref)
        u = lax.dot_general(v_ref[...], ab[rows, :], (((1,), (0,)), ((), ())), precision=HI, preferred_element_type=jnp.float32)
        ab[rows, :] = u
        lhs = ab[rows, 0:NB]
        blk = lax.broadcasted_iota(jnp.int32, (TILE, NB), 1) // TILE
        lhs = jnp.where(blk > t, lhs, 0.0)
        prod = lax.dot_general(lhs, u, (((0,), (0,)), ((), ())), precision=HI, preferred_element_type=jnp.float32)
        ab[...] = ab[...] - prod
        return 0

    lax.fori_loop(0, NB // TILE, step, 0)


def eye_into(ref):
    r = lax.broadcasted_iota(jnp.int32, (NB, NB), 0)
    c = lax.broadcasted_iota(jnp.int32, (NB, NB), 1)
    ref[...] = jnp.where(r == c, 1.0, 0.0).astype(jnp.float32)


def factor_kernel(d11, d21, d22, ab1, y_ref, ab2, t_ref, v_ref):
    ab1[:, 0:NB] = d11[...]
    eye_into(ab1.at[:, NB : 2 * NB])
    eye_into(ab2.at[:, NB : 2 * NB])
    factor_block(ab1, t_ref, v_ref)
    y_ref[...] = lax.dot_general(ab1[:, NB : 2 * NB], d21[...], (((1,), (1,)), ((), ())), precision=HI, preferred_element_type=jnp.float32)
    ab2[:, 0:NB] = d22[...] - lax.dot_general(y_ref[...], y_ref[...], (((0,), (0,)), ((), ())), precision=HI, preferred_element_type=jnp.float32)
    factor_block(ab2, t_ref, v_ref)


def factors(d11, d21, d22):
    f = jnp.float32
    vm = pl.BlockSpec(memory_space=pltpu.VMEM)
    return pl.pallas_call(
        factor_kernel,
        out_shape=[jax.ShapeDtypeStruct((NB, 2 * NB), f), jax.ShapeDtypeStruct((NB, NB), f), jax.ShapeDtypeStruct((NB, 2 * NB), f)],
        in_specs=[vm] * 3, out_specs=[vm] * 3,
        scratch_shapes=[pltpu.VMEM((TILE, TILE), f), pltpu.VMEM((TILE, TILE), f)],
        name="factors",
    )(d11, d21, d22)


def split(v):
    hi = v.astype(jnp.bfloat16)
    return hi, (v - hi.astype(jnp.float32)).astype(jnp.bfloat16)


def dot3(a, b, ca, cb):
    dims = (((ca,), (cb,)), ((), ()))
    f = lambda p, q: lax.dot_general(p, q, dims, preferred_element_type=jnp.float32)
    return f(a[1], b[0]) + f(a[0], b[1]) + f(a[0], b[0])


HR = 256


def update_kernel(pos, m, rp, cp, ab1, y, ab2, out, wh, wl, l1h, l1l, l2h, l2l, yh, yl, low):
    g = pl.program_id(0)
    k, r, c = pos[0], pos[1], pos[2]

    @pl.when(g == 0)
    def _():
        l1 = split(ab1[:, NB : 2 * NB])
        l2 = split(ab2[:, NB : 2 * NB])
        ys = split(y[...])
        l1h[...], l1l[...] = l1
        l2h[...], l2l[...] = l2
        yh[...], yl[...] = ys
        tri = lax.broadcasted_iota(jnp.int32, (NB, NB), 0) <= lax.broadcasted_iota(jnp.int32, (NB, NB), 1)
        for p, (ab, mod) in enumerate(((ab1, k), (ab2, k + 1))):
            @pl.when(c == lax.rem(mod, 16))
            def _():
                low[p] = jnp.where(tri, ab[:, 0:NB], 0.0).T
        for j in range(2):
            for h in range(2):
                cols = slice(j * NB + h * 256, j * NB + h * 256 + 256)
                a = [jnp.concatenate([cp[p, pl.ds(2 * t + j, NB, stride=8), :] for t in (2 * h, 2 * h + 1)], axis=1) for p in range(2)]
                w = jnp.where(16 * j + c > k, dot3(l1, split(a[0]), 1, 0), 0.0)
                ws = split(w)
                s = a[1] - dot3(ys, ws, 0, 0)
                w2 = jnp.where(16 * j + c > k + 1, dot3(l2, split(s), 1, 0), 0.0)
                wh[0:NB, cols], wl[0:NB, cols] = ws
                wh[NB : 2 * NB, cols], wl[NB : 2 * NB, cols] = split(w2)

    i, half = g // 2, lax.rem(g, 2)
    row = 8 * i + r

    @pl.when(row <= k)
    def _():
        out[...] = m[...]

    @pl.when(row > k)
    def _():
        xa = dot3(split(rp[0, 0]), (l1h[...], l1l[...]), 1, 1)
        xs = split(xa)
        s = rp[1, 0] - dot3(xs, (yh[...], yl[...]), 1, 0)
        x2 = jnp.where(row > k + 1, dot3(split(s), (l2h[...], l2l[...]), 1, 1), 0.0)
        x2s = split(x2)
        left = tuple(jnp.concatenate([a, b], axis=1) for a, b in zip(xs, x2s))
        for j in range(2):
            for h in range(2):
                cols = slice(j * NB + h * 256, j * NB + h * 256 + 256)
                prod = dot3(left, (wh[:, cols], wl[:, cols]), 1, 0)
                for t in range(2):
                    rows = pl.ds(2 * (2 * h + t) + j, HR, stride=8)
                    out[rows, :] = m[rows, :] - prod[:, t * 128 : t * 128 + 128]
        for x, kk in ((xa, k), (x2, k + 1)):
            @pl.when(jnp.logical_and(c == lax.rem(kk, 16), row > kk))
            def _():
                for t in range(4):
                    out[pl.ds(2 * t + kk // 16, HR, stride=8), :] = x[:, t * 128 : t * 128 + 128]

    for p in range(2):
        kk = k + p

        @pl.when(jnp.logical_and(c == lax.rem(kk, 16), row == kk))
        def _():
            for t in range(4):
                out[pl.ds(2 * t + kk // 16, HR, stride=8), :] = low[p, pl.ds(pl.multiple_of(half * HR, HR), HR), t * 128 : t * 128 + 128]


def update(pos, m, rp, cp, ab1, y, ab2):
    full = lambda *s: pl.BlockSpec(s, lambda g: (0,) * len(s))
    b = jnp.bfloat16
    return pl.pallas_call(
        update_kernel,
        grid=(8,),
        out_shape=jax.ShapeDtypeStruct((16384, 128), jnp.float32),
        in_specs=[
            pl.BlockSpec(memory_space=pltpu.SMEM),
            pl.BlockSpec((8 * HR, 128), lambda g: (g, 0)),
            pl.BlockSpec((2, 1, HR, NB), lambda g: (0, g // 2, g % 2, 0)),
            full(2, 4096, 128), full(NB, 2 * NB), full(NB, NB), full(NB, 2 * NB),
        ],
        out_specs=pl.BlockSpec((8 * HR, 128), lambda g: (g, 0)),
        scratch_shapes=[pltpu.VMEM((2 * NB, 2 * NB), b), pltpu.VMEM((2 * NB, 2 * NB), b)] + [pltpu.VMEM((NB, NB), b)] * 6 + [pltpu.VMEM((2, NB, NB), jnp.float32)],
        compiler_params=pltpu.CompilerParams(vmem_limit_bytes=56 * 2**20),
        name="trailing",
    )(pos, m, rp, cp, ab1, y, ab2)


def per_device(matrix_in, panel_start):
    k = panel_start[0]
    flat = matrix_in.reshape(4, NB, 2, 4, 128).transpose(0, 1, 3, 2, 4).reshape(16384, 128)
    rp, cp, g = lax.switch(k, [functools.partial(gather, kk) for kk in range(30)], flat)
    ab1, y, ab2 = factors(g[0], g[1], g[2])
    pos = jnp.stack([k, lax.axis_index("row"), lax.axis_index("col")]).astype(jnp.int32)
    out = update(pos, flat, rp, cp, ab1, y, ab2)
    return out.reshape(4, NB, 4, 2, 128).transpose(0, 1, 3, 2, 4).reshape(4, NB, 2, NB)


def solution(mesh):
    return jax.shard_map(
        per_device,
        mesh=mesh,
        in_specs=(P(None, "row", None, "col"), P()),
        out_specs=P(None, "row", None, "col"),
        check_vma=False,
    )
```

```python
import functools

import jax
import jax.numpy as jnp
from jax import lax
from jax.experimental import pallas as pl
from jax.experimental.pallas import tpu as pltpu
from jax.sharding import PartitionSpec as P

MESH = pl.DeviceIdType.MESH
HI = lax.Precision.HIGHEST
NB = 512
TILE = 128
GR = TILE // 8


R = 32
CPB = 128 // R
YR = 512
NY = 2048 // YR
RG = 64
CG = 128 // RG
LAG = 2


def both(*terms):
    return functools.reduce(jnp.logical_and, terms)


def loop(n, body):
    def run(i, carry):
        body(i)
        return carry

    lax.fori_loop(0, n, run, 0)


def comm_kernel(k, m_hbm, rp, cp, g, mbuf, ld_sem, cl_sem, pr_sem, ps_sem, yr_sem, ys_sem, yd_sem, yds_sem, gr_sem, gs_sem, gd_sem, gds_sem, place, hop):
    r, c = lax.axis_index("row"), lax.axis_index("col")
    y, core = r // 2, lax.rem(r, 2)
    x, z = c // 4, lax.rem(c, 4)
    partner = (r + 1 - 2 * core, c)

    def plane(axis, sig):
        return (r, lax.rem(x + sig * (1 - axis) + 4, 4) * 4 + lax.rem(z + sig * axis + 4, 4))

    def along(sig):
        return (lax.rem(y + sig + 4, 4) * 2 + core, c)

    barrier = pltpu.get_barrier_semaphore()
    for nb in (plane(0, 1), plane(0, -1), plane(1, 1), plane(1, -1), along(1), along(-1), partner):
        pl.semaphore_signal(barrier, inc=1, device_id=nb, device_id_type=MESH)

    ks = (k, k + 1)
    own_c = [kk % 16 for kk in ks]
    own_j = [kk // 16 for kk in ks]
    own_r = [kk % 8 for kk in ks]
    own_i = [kk // 8 for kk in ks]
    nblk = [4 - i for i in own_i]
    is_c = [c == v for v in own_c]
    is_r = [r == v for v in own_r]

    def pick(p, v):
        return v[0] if v[0] == v[1] else jnp.where(p == 0, v[0], v[1])

    def copy(src, dst, ssem, rsem, dev):
        return pltpu.make_async_remote_copy(src_ref=src, dst_ref=dst, send_sem=ssem, recv_sem=rsem, device_id=dev, device_id_type=MESH)

    def load():
        rest = pl.ds(own_i[0] * 4096, (4 - own_i[0]) * 4096)
        return pltpu.make_async_copy(m_hbm.at[rest, :], mbuf.at[rest, :], ld_sem)

    def slab(p):
        return pltpu.make_async_copy(m_hbm.at[pl.ds(own_i[p] * 4096, 4096), :], cp.at[p], cl_sem.at[p])

    def spread(p, i, dst):
        def group(q):
            for l in range(4):
                dst[pl.ds(pl.multiple_of(q * 64, 64), 64), l * 128 : l * 128 + 128] = mbuf[pl.ds(i * 4096 + q * 512 + 2 * l + pick(p, own_j), 64, stride=8), :]

        loop(8, group)

    def common(gi):
        return jnp.where(gi == 0, 0, 1), jnp.where(gi == 2, 1, 0)

    for p in range(2):
        pl.when(is_r[p])(lambda p=p: slab(p).start())

    @pl.when(jnp.logical_or(is_c[0], is_c[1]))
    def _():
        load().start()
        load().wait()

        def first(gi):
            o, p = common(gi)

            @pl.when(both(r == pick(o, own_r), c == pick(p, own_c)))
            def _():
                spread(p, pick(o, own_i), g.at[gi])

        loop(3, first)

    for p in range(2):
        pl.when(is_r[p])(lambda p=p: slab(p).wait())
    pl.semaphore_wait(barrier, 7)

    def placing(n):
        p, t = n // 4, lax.rem(n, 4)
        sig, axis = 1 - 2 * lax.rem(t, 2), t // 2
        dx = lax.rem(sig * (x - pick(p, [v // 4 for v in own_c])) + 8, 4)
        dz = lax.rem(sig * (z - pick(p, [v % 4 for v in own_c])) + 8, 4)
        a, b = jnp.where(axis == 0, dx, dz), jnp.where(axis == 0, dz, dx)
        place[n, 0] = LAG * jnp.where(both(a == 0, b != 0), 4 + b, a + b)
        place[n, 1] = jnp.where(jnp.logical_or(both(b == 0, a < 3), both(b != 0, a == 3)), 1, 0)
        place[n, 2] = jnp.where(both(a != 0, b < 3), 1, 0)
        place[n, 3] = plane(axis, sig)[1]
        place[n, 4] = plane(1 - axis, sig)[1]

    loop(8, placing)
    for p in range(2):
        for d in range(2):
            hop[2 * p + d] = LAG * lax.rem((1 - 2 * d) * (y - own_r[p] // 2) + 8, 4)

    def chunk(p, t, ch):
        row = pl.multiple_of(t * 128 + lax.rem(ch, CPB) * R, R)
        return rp.at[p, pick(p, own_i) + ch // CPB, pl.ds(row, R), :]

    def gchunk(gi, t, q):
        return g.at[gi, pl.ds(pl.multiple_of(t * 128 + q * RG, RG), RG), :]

    def ychunk(p, d, u):
        return cp.at[p, pl.ds(pl.multiple_of(d * 2048 + u * YR, YR), YR), :]

    steps = max(max(nblk) * CPB + 7 * LAG, CG + 10 * LAG, NY + 3 * LAG)

    def step(s):
        def block(idx):
            gi, t = idx // 4, lax.rem(idx, 4)
            o, p = common(gi)
            n = 4 * p + t
            depth = place[n, 0]
            dy = hop[2 * o + lax.rem(t, 2)]
            q = s - depth - dy

            @pl.when(both(q >= 0, q < CG, core == pick(o, [v % 2 for v in own_r])))
            def _():
                sl = gchunk(gi, t, q)

                @pl.when(depth + dy > 0)
                def _():
                    copy(sl, sl, gs_sem.at[gi, t, 0], gr_sem.at[gi, t, q], partner).wait_recv()

                up = along(1 - 2 * lax.rem(t, 2))
                for w, cond, dev in ((0, place[n, 1] > 0, (r, place[n, 3])), (1, place[n, 2] > 0, (r, place[n, 4])), (1, both(depth == 0, dy < 3 * LAG), up)):
                    @pl.when(cond)
                    def _():
                        copy(sl, sl, gs_sem.at[gi, t, w], gr_sem.at[gi, t, q], dev).start()

                copy(sl, sl, gds_sem.at[gi], gd_sem.at[gi], partner).start()

        @pl.when(s < CG + 10 * LAG)
        def _():
            loop(12, block)

        def strip(idx):
            p, t = idx // 4, lax.rem(idx, 4)
            depth = place[idx, 0]
            ch = s - depth

            @pl.when(both(ch >= 0, ch < pick(p, nblk) * CPB))
            def _():
                sl = chunk(p, t, ch)

                @pl.when(depth > 0)
                def _():
                    copy(sl, sl, ps_sem.at[p, t, 0], pr_sem.at[p, t, ch], partner).wait_recv()

                for w, (cond, dev) in enumerate(((place[idx, 1] > 0, (r, place[idx, 3])), (place[idx, 2] > 0, (r, place[idx, 4])))):
                    @pl.when(cond)
                    def _():
                        copy(sl, sl, ps_sem.at[p, t, w], pr_sem.at[p, t, ch], dev).start()

        loop(8, strip)

        def rows(idx):
            p, d = idx // 2, lax.rem(idx, 2)
            dy = hop[idx]
            u = s - dy

            @pl.when(both(u >= 0, u < NY, core == pick(p, [v % 2 for v in own_r])))
            def _():
                sl = ychunk(p, d, u)

                @pl.when(dy > 0)
                def _():
                    copy(sl, sl, ys_sem.at[p, d], yr_sem.at[p, d, u], partner).wait_recv()

                @pl.when(dy < 3 * LAG)
                def _():
                    copy(sl, sl, ys_sem.at[p, d], yr_sem.at[p, d, u], along(1 - 2 * d)).start()

                copy(sl, sl, yds_sem.at[p], yd_sem.at[p], partner).start()

        @pl.when(s < NY + 3 * LAG)
        def _():
            loop(4, rows)

        @pl.when(both(jnp.logical_or(is_c[0], is_c[1]), lax.rem(s + 1, CPB) == 0))
        def _():
            p = jnp.where(is_c[0], 0, 1)
            b = (s + 1) // CPB

            @pl.when(b < pick(p, nblk))
            def _():
                i = pick(p, own_i) + b
                spread(p, i, rp.at[p, i])

    loop(steps + 1, lambda s: step(s - 1))

    def tail_rows(p):
        mine = core == pick(p, [v % 2 for v in own_r])
        whole = copy(cp.at[p], cp.at[p], yds_sem.at[p], yd_sem.at[p], partner)
        pl.when(jnp.logical_not(mine))(whole.wait_recv)

        @pl.when(mine)
        def _():
            whole.wait_send()
            for d in range(2):
                half = cp.at[p, pl.ds(d * 2048, 2048), :]
                pl.when(hop[2 * p + d] < 3 * LAG)(copy(half, half, ys_sem.at[p, d], yd_sem.at[p], partner).wait_send)

    loop(2, tail_rows)

    def tail_block(gi):
        o, p = common(gi)
        mine = core == pick(o, [v % 2 for v in own_r])
        whole = copy(g.at[gi], g.at[gi], gds_sem.at[gi], gd_sem.at[gi], partner)
        pl.when(jnp.logical_not(mine))(whole.wait_recv)

        @pl.when(mine)
        def _():
            whole.wait_send()

            def one(t):
                n = 4 * p + t
                part = g.at[gi, pl.ds(0, 128), :]
                for w, cond in enumerate((place[n, 1] > 0, jnp.logical_or(place[n, 2] > 0, both(place[n, 0] == 0, hop[2 * o + lax.rem(t, 2)] < 3 * LAG)))):
                    pl.when(cond)(copy(part, part, gs_sem.at[gi, t, w], gd_sem.at[gi], partner).wait_send)

            loop(4, one)

    loop(3, tail_block)

    for p in range(2):
        def tail_strip(t, p=p):
            part = rp.at[p, pl.ds(0, nblk[p]), pl.ds(0, 128), :]
            for w, cond in enumerate((place[4 * p + t, 1] > 0, place[4 * p + t, 2] > 0)):
                pl.when(cond)(copy(part, part, ps_sem.at[p, t, w], pr_sem.at[p, t, 0], partner).wait_send)

        loop(4, tail_strip)


def gather(k, m_flat):
    f = jnp.float32
    vm = pl.BlockSpec(memory_space=pltpu.VMEM)
    dma = pltpu.SemaphoreType.DMA
    return pl.pallas_call(
        functools.partial(comm_kernel, k),
        out_shape=[jax.ShapeDtypeStruct((2, 4, NB, NB), f), jax.ShapeDtypeStruct((2, 4096, 128), f), jax.ShapeDtypeStruct((3, NB, NB), f)],
        in_specs=[pl.BlockSpec(memory_space=pl.ANY)], out_specs=[vm] * 3,
        scratch_shapes=[pltpu.VMEM((16384, 128), f), dma, dma((2,)),
                        dma((2, 4, (4 - k // 8) * CPB)), dma((2, 4, 2)), dma((2, 2, NY)), dma((2, 2)), dma((2,)), dma((2,)),
                        dma((3, 4, CG)), dma((3, 4, 2)), dma((3,)), dma((3,)),
                        pltpu.SMEM((8, 5), jnp.int32), pltpu.SMEM((4,), jnp.int32)],
        compiler_params=pltpu.CompilerParams(collective_id=k, has_side_effects=True, vmem_limit_bytes=40 * 2**20),
        name="gather",
    )(m_flat)


def rep(v, i):
    return jnp.broadcast_to(v[i : i + 1, :], v.shape)


def lane(v, l):
    return jnp.broadcast_to(v[:, l : l + 1], v.shape)


def tile_factor(t_ref, v_ref):
    sub = lax.broadcasted_iota(jnp.int32, (8, TILE), 0)
    lan = lax.broadcasted_iota(jnp.int32, (8, TILE), 1)
    for g in range(GR):
        v_ref[8 * g : 8 * g + 8, :] = jnp.where(lan == sub + 8 * g, 1.0, 0.0).astype(jnp.float32)
    first = t_ref[0:8, :]
    e = [lane(first, c) for c in range(8)]
    for g in range(GR):
        rows = slice(8 * g, 8 * g + 8)
        t = t_ref[rows, :]
        v = v_ref[rows, :]
        if g + 1 < GR:
            raw = t_ref[8 * g + 8 : 8 * g + 16, :]
            f_next = [lane(raw, 8 * g + c) for c in range(8)]
            e_next = [lane(raw, 8 * g + 8 + c) for c in range(8)]
        s, u, low = [], {}, []
        for j in range(8):
            sj = lax.rsqrt(rep(e[j], j))
            col = e[j] * sj
            s.append(sj)
            for c in range(j + 1, 8):
                u[j, c] = rep(e[j], c) * sj
                e[c] = e[c] - col * u[j, c]
            low.append(jnp.where(sub > j, col, 0.0))
        if g + 1 < GR:
            for j in range(8):
                f_next[j] = f_next[j] * s[j]
                for c in range(j + 1, 8):
                    f_next[c] = f_next[c] - f_next[j] * u[j, c]
                for c in range(8):
                    e_next[c] = e_next[c] - f_next[j] * rep(f_next[j], c)
        for j in range(8):
            rt = rep(t, j) * s[j]
            rv = rep(v, j) * s[j]
            t = jnp.where(sub == j, rt, t - low[j] * rt)
            v = jnp.where(sub == j, rv, v - low[j] * rv)
        t_ref[rows, :] = t
        v_ref[rows, :] = v
        rts = [rep(t, c) for c in range(8)]
        rvs = [rep(v, c) for c in range(8)]
        for h in range(g + 1, GR):
            hr = slice(8 * h, 8 * h + 8)
            th = t_ref[hr, :]
            vh = v_ref[hr, :]
            f = f_next if h == g + 1 else [lane(th, 8 * g + c) for c in range(8)]
            for j in range(8):
                if h > g + 1:
                    f[j] = f[j] * s[j]
                    for c in range(j + 1, 8):
                        f[c] = f[c] - f[j] * u[j, c]
                th = th - f[j] * rts[j]
                vh = vh - f[j] * rvs[j]
            t_ref[hr, :] = th
            v_ref[hr, :] = vh
        if g + 1 < GR:
            e = e_next


def mm(a, b, ca, cb):
    return lax.dot_general(a, b, (((ca,), (cb,)), ((), ())), precision=HI, preferred_element_type=jnp.float32)


def factor_block(ab, t_ref, v_ref):
    last = NB // TILE - 1

    def step(t, _):
        rows = pl.ds(pl.multiple_of(t * TILE, TILE), TILE)
        t_ref[...] = ab[rows, rows]
        tile_factor(t_ref, v_ref)
        ab[rows, rows] = t_ref[...]
        ab[rows, pl.ds(pl.multiple_of(NB + t * TILE, TILE), TILE)] = v_ref[...]
        for tt in range(last + 1):
            here = slice(tt * TILE, tt * TILE + TILE)
            below = slice(tt * TILE + TILE, NB)

            @pl.when(t == tt)
            def _():
                v = v_ref[...]
                if tt:
                    w = mm(v, ab[here, NB : NB + tt * TILE], 1, 0)
                    ab[here, NB : NB + tt * TILE] = w
                if tt < last:
                    u = mm(v, ab[here, below], 1, 0)
                    ab[here, below] = u
                    ab[below, below] = ab[below, below] - mm(u, u, 0, 0)
                    inv = slice(NB, NB + tt * TILE + TILE)
                    ab[below, inv] = ab[below, inv] - mm(u, ab[here, inv], 0, 0)
        return 0

    lax.fori_loop(0, last + 1, step, 0)


def eye_into(ref):
    r = lax.broadcasted_iota(jnp.int32, (NB, NB), 0)
    c = lax.broadcasted_iota(jnp.int32, (NB, NB), 1)
    ref[...] = jnp.where(r == c, 1.0, 0.0).astype(jnp.float32)


def factor_kernel(g, both_ab, y_ref, t_ref, v_ref):
    def panel(p, carry):
        ab = both_ab.at[p]
        eye_into(ab.at[:, NB : 2 * NB])

        @pl.when(p == 0)
        def _():
            ab[:, 0:NB] = g[0]

        @pl.when(p == 1)
        def _():
            for q in range(4):
                here = slice(q * TILE, q * TILE + TILE)
                y_ref[here, :] = mm(both_ab[0, here, NB : NB + q * TILE + TILE], g[1, :, 0 : q * TILE + TILE], 1, 1)
            for q in range(4):
                here, right = slice(q * TILE, q * TILE + TILE), slice(q * TILE, NB)
                ab[here, right] = g[2, here, right] - mm(y_ref[:, here], y_ref[:, right], 0, 0)

        factor_block(ab, t_ref, v_ref)
        return carry

    lax.fori_loop(0, 2, panel, 0)


def factors(g):
    f = jnp.float32
    vm = pl.BlockSpec(memory_space=pltpu.VMEM)
    return pl.pallas_call(
        factor_kernel,
        out_shape=[jax.ShapeDtypeStruct((2, NB, 2 * NB), f), jax.ShapeDtypeStruct((NB, NB), f)],
        in_specs=[vm], out_specs=[vm] * 2,
        scratch_shapes=[pltpu.VMEM((TILE, TILE), f), pltpu.VMEM((TILE, TILE), f)],
        name="factors",
    )(g)


def split(v):
    hi = v.astype(jnp.bfloat16)
    return hi, (v - hi.astype(jnp.float32)).astype(jnp.bfloat16)


def dot3(a, b, ca, cb):
    dims = (((ca,), (cb,)), ((), ()))
    f = lambda p, q: lax.dot_general(p, q, dims, preferred_element_type=jnp.float32)
    return f(a[1], b[0]) + f(a[0], b[1]) + f(a[0], b[0])


HR = 256


def tri3(a, low, ca):
    h = NB // 2
    if ca == 1:
        first = dot3([v[:, :h] for v in a], [v[:h, :h] for v in low], 1, 1)
        return jnp.concatenate([first, dot3(a, [v[h:, :] for v in low], 1, 1)], axis=1)
    first = dot3([v[:h, :h] for v in low], [v[:h, :] for v in a], 1, 0)
    return jnp.concatenate([first, dot3([v[h:, :] for v in low], a, 1, 0)], axis=0)


def update_kernel(pos, m, rp, cp, ab, y, out, wh, wl, l1h, l1l, l2h, l2l, yh, yl, low, lh, ll):
    g = pl.program_id(0)
    k, r, c = pos[0], pos[1], pos[2]

    @pl.when(g == 0)
    def _():
        l1h[...], l1l[...] = split(ab[0, :, NB : 2 * NB])
        l2h[...], l2l[...] = split(ab[1, :, NB : 2 * NB])
        yh[...], yl[...] = split(y[...])
        tri = lax.broadcasted_iota(jnp.int32, (NB, NB), 0) <= lax.broadcasted_iota(jnp.int32, (NB, NB), 1)
        def lower(p):
            @pl.when(c == lax.rem(k + p, 16))
            def _():
                low[p] = jnp.where(tri, ab[p, :, 0:NB], 0.0).T

        loop(2, lower)

        def columns(q):
            j, h = q // 2, lax.rem(q, 2)

            @pl.when(16 * j + c > k)
            def _():
                    cols = pl.ds(pl.multiple_of(q * 256, 256), 256)
                    a = [jnp.concatenate([cp[p, pl.ds(4 * h + 2 * t + j, NB, stride=8), :] for t in (0, 1)], axis=1) for p in range(2)]
                    ws = split(tri3(split(a[0]), (l1h[...], l1l[...]), 0))
                    s = a[1] - dot3((yh[...], yl[...]), ws, 0, 0)
                    w2 = jnp.where(16 * j + c > k + 1, tri3(split(s), (l2h[...], l2l[...]), 0), 0.0)
                    wh[0:NB, cols], wl[0:NB, cols] = ws
                    wh[NB : 2 * NB, cols], wl[NB : 2 * NB, cols] = split(w2)

        loop(4, columns)

    i, half = g // 2, lax.rem(g, 2)
    row = 8 * i + r

    @pl.when(row <= k)
    def _():
        out[...] = m[...]

    @pl.when(row > k)
    def _():
        xa = tri3(split(rp[0, 0]), (l1h[...], l1l[...]), 1)
        xs = split(xa)
        s = rp[1, 0] - dot3(xs, (yh[...], yl[...]), 1, 0)
        x2 = jnp.where(row > k + 1, tri3(split(s), (l2h[...], l2l[...]), 1), 0.0)
        x2s = split(x2)
        lh[:, 0:NB], ll[:, 0:NB] = xs
        lh[:, NB : 2 * NB], ll[:, NB : 2 * NB] = x2s

        def columns(q):
            j, h = q // 2, lax.rem(q, 2)

            @pl.when(16 * j + c <= k)
            def _():
                for t in range(2):
                    rows = pl.ds(4 * h + 2 * t + j, HR, stride=8)
                    out[rows, :] = m[rows, :]

            @pl.when(16 * j + c > k)
            def _():
                cols = pl.ds(pl.multiple_of(q * 256, 256), 256)
                prod = dot3((lh[...], ll[...]), (wh[:, cols], wl[:, cols]), 1, 0)
                for t in range(2):
                    rows = pl.ds(4 * h + 2 * t + j, HR, stride=8)
                    out[rows, :] = m[rows, :] - prod[:, t * 128 : t * 128 + 128]

        loop(4, columns)

        for x, kk in ((xa, k), (x2, k + 1)):
            @pl.when(jnp.logical_and(c == lax.rem(kk, 16), row > kk))
            def _():
                for t in range(4):
                    out[pl.ds(2 * t + kk // 16, HR, stride=8), :] = x[:, t * 128 : t * 128 + 128]

    for p in range(2):
        kk = k + p

        @pl.when(jnp.logical_and(c == lax.rem(kk, 16), row == kk))
        def _():
            for t in range(4):
                out[pl.ds(2 * t + kk // 16, HR, stride=8), :] = low[p, pl.ds(pl.multiple_of(half * HR, HR), HR), t * 128 : t * 128 + 128]


def update(pos, m, rp, cp, ab, y):
    full = lambda *s: pl.BlockSpec(s, lambda g: (0,) * len(s))
    b = jnp.bfloat16
    return pl.pallas_call(
        update_kernel,
        grid=(8,),
        out_shape=jax.ShapeDtypeStruct((16384, 128), jnp.float32),
        in_specs=[
            pl.BlockSpec(memory_space=pltpu.SMEM),
            pl.BlockSpec((8 * HR, 128), lambda g: (g, 0)),
            pl.BlockSpec((2, 1, HR, NB), lambda g: (0, g // 2, g % 2, 0)),
            full(2, 4096, 128), full(2, NB, 2 * NB), full(NB, NB),
        ],
        out_specs=pl.BlockSpec((8 * HR, 128), lambda g: (g, 0)),
        scratch_shapes=[pltpu.VMEM((2 * NB, 2 * NB), b), pltpu.VMEM((2 * NB, 2 * NB), b)] + [pltpu.VMEM((NB, NB), b)] * 6 + [pltpu.VMEM((2, NB, NB), jnp.float32), pltpu.VMEM((HR, 2 * NB), b), pltpu.VMEM((HR, 2 * NB), b)],
        compiler_params=pltpu.CompilerParams(vmem_limit_bytes=56 * 2**20),
        name="trailing",
    )(pos, m, rp, cp, ab, y)


def per_device(matrix_in, panel_start):
    k = panel_start[0]
    flat = matrix_in.reshape(4, NB, 2, 4, 128).transpose(0, 1, 3, 2, 4).reshape(16384, 128)
    rp, cp, g = lax.switch(k, [functools.partial(gather, kk) for kk in range(30)], flat)
    ab, y = factors(g)
    pos = jnp.stack([k, lax.axis_index("row"), lax.axis_index("col")]).astype(jnp.int32)
    out = update(pos, flat, rp, cp, ab, y)
    return out.reshape(4, NB, 4, 2, 128).transpose(0, 1, 3, 2, 4).reshape(4, NB, 2, NB)


def solution(mesh):
    return jax.shard_map(
        per_device,
        mesh=mesh,
        in_specs=(P(None, "row", None, "col"), P()),
        out_specs=P(None, "row", None, "col"),
        check_vma=False,
    )
```

```python
import functools

import jax
import jax.numpy as jnp
from jax import lax
from jax.experimental import pallas as pl
from jax.experimental.pallas import tpu as pltpu
from jax.sharding import PartitionSpec as P

MESH = pl.DeviceIdType.MESH
HI = lax.Precision.HIGHEST
NB = 512
TILE = 128
GR = TILE // 8


R = 32
CPB = 128 // R
YR = 512
NY = 2048 // YR
RG = 64
CG = 128 // RG
LAG = 2


def both(*terms):
    return functools.reduce(jnp.logical_and, terms)


def loop(n, body):
    def run(i, carry):
        body(i)
        return carry

    lax.fori_loop(0, n, run, 0)


def comm_kernel(k, m_hbm, rp, cp, g, mbuf, ld_sem, cl_sem, pr_sem, ps_sem, yr_sem, ys_sem, yd_sem, yds_sem, gr_sem, gs_sem, gd_sem, gds_sem, place, hop):
    r, c = lax.axis_index("row"), lax.axis_index("col")
    y, core = r // 2, lax.rem(r, 2)
    x, z = c // 4, lax.rem(c, 4)
    partner = (r + 1 - 2 * core, c)

    def plane(axis, sig):
        return (r, lax.rem(x + sig * (1 - axis) + 4, 4) * 4 + lax.rem(z + sig * axis + 4, 4))

    def along(sig):
        return (lax.rem(y + sig + 4, 4) * 2 + core, c)

    barrier = pltpu.get_barrier_semaphore()
    for nb in (plane(0, 1), plane(0, -1), plane(1, 1), plane(1, -1), along(1), along(-1), partner):
        pl.semaphore_signal(barrier, inc=1, device_id=nb, device_id_type=MESH)

    ks = (k, k + 1)
    own_c = [kk % 16 for kk in ks]
    own_j = [kk // 16 for kk in ks]
    own_r = [kk % 8 for kk in ks]
    own_i = [kk // 8 for kk in ks]
    nblk = [4 - i for i in own_i]
    is_c = [c == v for v in own_c]
    is_r = [r == v for v in own_r]

    def pick(p, v):
        return v[0] if v[0] == v[1] else jnp.where(p == 0, v[0], v[1])

    def copy(src, dst, ssem, rsem, dev):
        return pltpu.make_async_remote_copy(src_ref=src, dst_ref=dst, send_sem=ssem, recv_sem=rsem, device_id=dev, device_id_type=MESH)

    def load():
        rest = pl.ds(own_i[0] * 4096, (4 - own_i[0]) * 4096)
        return pltpu.make_async_copy(m_hbm.at[rest, :], mbuf.at[rest, :], ld_sem)

    def slab(p):
        return pltpu.make_async_copy(m_hbm.at[pl.ds(own_i[p] * 4096, 4096), :], cp.at[p], cl_sem.at[p])

    def spread(p, i, dst):
        def group(q):
            for l in range(4):
                dst[pl.ds(pl.multiple_of(q * 64, 64), 64), l * 128 : l * 128 + 128] = mbuf[pl.ds(i * 4096 + q * 512 + 2 * l + pick(p, own_j), 64, stride=8), :]

        loop(8, group)

    def common(gi):
        return jnp.where(gi == 0, 0, 1), jnp.where(gi == 2, 1, 0)

    for p in range(2):
        pl.when(is_r[p])(lambda p=p: slab(p).start())

    @pl.when(jnp.logical_or(is_c[0], is_c[1]))
    def _():
        load().start()
        load().wait()

        def first(gi):
            o, p = common(gi)

            @pl.when(both(r == pick(o, own_r), c == pick(p, own_c)))
            def _():
                spread(p, pick(o, own_i), g.at[gi])

        loop(3, first)

    for p in range(2):
        pl.when(is_r[p])(lambda p=p: slab(p).wait())
    pl.semaphore_wait(barrier, 7)

    def placing(n):
        p, t = n // 4, lax.rem(n, 4)
        sig, axis = 1 - 2 * lax.rem(t, 2), t // 2
        dx = lax.rem(sig * (x - pick(p, [v // 4 for v in own_c])) + 8, 4)
        dz = lax.rem(sig * (z - pick(p, [v % 4 for v in own_c])) + 8, 4)
        a, b = jnp.where(axis == 0, dx, dz), jnp.where(axis == 0, dz, dx)
        place[n, 0] = LAG * jnp.where(both(a == 0, b != 0), 4 + b, a + b)
        place[n, 1] = jnp.where(jnp.logical_or(both(b == 0, a < 3), both(b != 0, a == 3)), 1, 0)
        place[n, 2] = jnp.where(both(a != 0, b < 3), 1, 0)
        place[n, 3] = plane(axis, sig)[1]
        place[n, 4] = plane(1 - axis, sig)[1]

    loop(8, placing)
    for p in range(2):
        for d in range(2):
            hop[2 * p + d] = LAG * lax.rem((1 - 2 * d) * (y - own_r[p] // 2) + 8, 4)

    def chunk(p, t, ch):
        row = pl.multiple_of(t * 128 + lax.rem(ch, CPB) * R, R)
        return rp.at[p, pick(p, own_i) + ch // CPB, pl.ds(row, R), :]

    def gchunk(gi, t, q):
        return g.at[gi, pl.ds(pl.multiple_of(t * 128 + q * RG, RG), RG), :]

    def ychunk(p, d, u):
        return cp.at[p, pl.ds(pl.multiple_of(d * 2048 + u * YR, YR), YR), :]

    steps = max(max(nblk) * CPB + 7 * LAG, CG + 10 * LAG, NY + 3 * LAG)

    def step(s):
        def block(idx):
            gi, t = idx // 4, lax.rem(idx, 4)
            o, p = common(gi)
            n = 4 * p + t
            depth = place[n, 0]
            dy = hop[2 * o + lax.rem(t, 2)]
            q = s - depth - dy

            @pl.when(both(q >= 0, q < CG, core == pick(o, [v % 2 for v in own_r])))
            def _():
                sl = gchunk(gi, t, q)

                @pl.when(depth + dy > 0)
                def _():
                    copy(sl, sl, gs_sem.at[gi, t, 0], gr_sem.at[gi, t, q], partner).wait_recv()

                up = along(1 - 2 * lax.rem(t, 2))
                for w, cond, dev in ((0, place[n, 1] > 0, (r, place[n, 3])), (1, place[n, 2] > 0, (r, place[n, 4])), (1, both(depth == 0, dy < 3 * LAG), up)):
                    @pl.when(cond)
                    def _():
                        copy(sl, sl, gs_sem.at[gi, t, w], gr_sem.at[gi, t, q], dev).start()

                copy(sl, sl, gds_sem.at[gi], gd_sem.at[gi], partner).start()

        @pl.when(s < CG + 10 * LAG)
        def _():
            loop(12, block)

        def strip(idx):
            p, t = idx // 4, lax.rem(idx, 4)
            depth = place[idx, 0]
            ch = s - depth

            @pl.when(both(ch >= 0, ch < pick(p, nblk) * CPB))
            def _():
                sl = chunk(p, t, ch)

                @pl.when(depth > 0)
                def _():
                    copy(sl, sl, ps_sem.at[p, t, 0], pr_sem.at[p, t, ch], partner).wait_recv()

                for w, (cond, dev) in enumerate(((place[idx, 1] > 0, (r, place[idx, 3])), (place[idx, 2] > 0, (r, place[idx, 4])))):
                    @pl.when(cond)
                    def _():
                        copy(sl, sl, ps_sem.at[p, t, w], pr_sem.at[p, t, ch], dev).start()

        loop(8, strip)

        def rows(idx):
            p, d = idx // 2, lax.rem(idx, 2)
            dy = hop[idx]
            u = s - dy

            @pl.when(both(u >= 0, u < NY, core == pick(p, [v % 2 for v in own_r])))
            def _():
                sl = ychunk(p, d, u)

                @pl.when(dy > 0)
                def _():
                    copy(sl, sl, ys_sem.at[p, d], yr_sem.at[p, d, u], partner).wait_recv()

                @pl.when(dy < 3 * LAG)
                def _():
                    copy(sl, sl, ys_sem.at[p, d], yr_sem.at[p, d, u], along(1 - 2 * d)).start()

                copy(sl, sl, yds_sem.at[p], yd_sem.at[p], partner).start()

        @pl.when(s < NY + 3 * LAG)
        def _():
            loop(4, rows)

        @pl.when(both(jnp.logical_or(is_c[0], is_c[1]), lax.rem(s + 1, CPB) == 0))
        def _():
            p = jnp.where(is_c[0], 0, 1)
            b = (s + 1) // CPB

            @pl.when(b < pick(p, nblk))
            def _():
                i = pick(p, own_i) + b
                spread(p, i, rp.at[p, i])

    loop(steps + 1, lambda s: step(s - 1))

    def tail_rows(p):
        mine = core == pick(p, [v % 2 for v in own_r])
        whole = copy(cp.at[p], cp.at[p], yds_sem.at[p], yd_sem.at[p], partner)
        pl.when(jnp.logical_not(mine))(whole.wait_recv)

        @pl.when(mine)
        def _():
            whole.wait_send()
            for d in range(2):
                half = cp.at[p, pl.ds(d * 2048, 2048), :]
                pl.when(hop[2 * p + d] < 3 * LAG)(copy(half, half, ys_sem.at[p, d], yd_sem.at[p], partner).wait_send)

    loop(2, tail_rows)

    def tail_block(gi):
        o, p = common(gi)
        mine = core == pick(o, [v % 2 for v in own_r])
        whole = copy(g.at[gi], g.at[gi], gds_sem.at[gi], gd_sem.at[gi], partner)
        pl.when(jnp.logical_not(mine))(whole.wait_recv)

        @pl.when(mine)
        def _():
            whole.wait_send()

            def one(t):
                n = 4 * p + t
                part = g.at[gi, pl.ds(0, 128), :]
                for w, cond in enumerate((place[n, 1] > 0, jnp.logical_or(place[n, 2] > 0, both(place[n, 0] == 0, hop[2 * o + lax.rem(t, 2)] < 3 * LAG)))):
                    pl.when(cond)(copy(part, part, gs_sem.at[gi, t, w], gd_sem.at[gi], partner).wait_send)

            loop(4, one)

    loop(3, tail_block)

    for p in range(2):
        def tail_strip(t, p=p):
            part = rp.at[p, pl.ds(0, nblk[p]), pl.ds(0, 128), :]
            for w, cond in enumerate((place[4 * p + t, 1] > 0, place[4 * p + t, 2] > 0)):
                pl.when(cond)(copy(part, part, ps_sem.at[p, t, w], pr_sem.at[p, t, 0], partner).wait_send)

        loop(4, tail_strip)


def gather(k, m_flat):
    f = jnp.float32
    vm = pl.BlockSpec(memory_space=pltpu.VMEM)
    dma = pltpu.SemaphoreType.DMA
    return pl.pallas_call(
        functools.partial(comm_kernel, k),
        out_shape=[jax.ShapeDtypeStruct((2, 4, NB, NB), f), jax.ShapeDtypeStruct((2, 4096, 128), f), jax.ShapeDtypeStruct((3, NB, NB), f)],
        in_specs=[pl.BlockSpec(memory_space=pl.ANY)], out_specs=[vm] * 3,
        scratch_shapes=[pltpu.VMEM((16384, 128), f), dma, dma((2,)),
                        dma((2, 4, (4 - k // 8) * CPB)), dma((2, 4, 2)), dma((2, 2, NY)), dma((2, 2)), dma((2,)), dma((2,)),
                        dma((3, 4, CG)), dma((3, 4, 2)), dma((3,)), dma((3,)),
                        pltpu.SMEM((8, 5), jnp.int32), pltpu.SMEM((4,), jnp.int32)],
        compiler_params=pltpu.CompilerParams(collective_id=k, has_side_effects=True, vmem_limit_bytes=21 * 2**20),
        name="gather",
    )(m_flat)


def rep(v, i):
    return jnp.broadcast_to(v[i : i + 1, :], v.shape)


def lane(v, l):
    return jnp.broadcast_to(v[:, l : l + 1], v.shape)


def tile_factor(t_ref, v_ref):
    sub = lax.broadcasted_iota(jnp.int32, (8, TILE), 0)
    lan = lax.broadcasted_iota(jnp.int32, (8, TILE), 1)
    for g in range(GR):
        v_ref[8 * g : 8 * g + 8, :] = jnp.where(lan == sub + 8 * g, 1.0, 0.0).astype(jnp.float32)
    first = t_ref[0:8, :]
    e = [lane(first, c) for c in range(8)]
    for g in range(GR):
        rows = slice(8 * g, 8 * g + 8)
        t = t_ref[rows, :]
        v = v_ref[rows, :]
        if g + 1 < GR:
            raw = t_ref[8 * g + 8 : 8 * g + 16, :]
            f_next = [lane(raw, 8 * g + c) for c in range(8)]
            e_next = [lane(raw, 8 * g + 8 + c) for c in range(8)]
        s, u, low = [], {}, []
        for j in range(8):
            sj = lax.rsqrt(rep(e[j], j))
            col = e[j] * sj
            s.append(sj)
            for c in range(j + 1, 8):
                u[j, c] = rep(e[j], c) * sj
                e[c] = e[c] - col * u[j, c]
            low.append(jnp.where(sub > j, col, 0.0))
        if g + 1 < GR:
            for j in range(8):
                f_next[j] = f_next[j] * s[j]
                for c in range(j + 1, 8):
                    f_next[c] = f_next[c] - f_next[j] * u[j, c]
                for c in range(8):
                    e_next[c] = e_next[c] - f_next[j] * rep(f_next[j], c)
        for j in range(8):
            rt = rep(t, j) * s[j]
            rv = rep(v, j) * s[j]
            t = jnp.where(sub == j, rt, t - low[j] * rt)
            v = jnp.where(sub == j, rv, v - low[j] * rv)
        t_ref[rows, :] = t
        v_ref[rows, :] = v
        rts = [rep(t, c) for c in range(8)]
        rvs = [rep(v, c) for c in range(8)]
        for h in range(g + 1, GR):
            hr = slice(8 * h, 8 * h + 8)
            th = t_ref[hr, :]
            vh = v_ref[hr, :]
            f = f_next if h == g + 1 else [lane(th, 8 * g + c) for c in range(8)]
            for j in range(8):
                if h > g + 1:
                    f[j] = f[j] * s[j]
                    for c in range(j + 1, 8):
                        f[c] = f[c] - f[j] * u[j, c]
                th = th - f[j] * rts[j]
                vh = vh - f[j] * rvs[j]
            t_ref[hr, :] = th
            v_ref[hr, :] = vh
        if g + 1 < GR:
            e = e_next


def mm(a, b, ca, cb):
    return lax.dot_general(a, b, (((ca,), (cb,)), ((), ())), precision=HI, preferred_element_type=jnp.float32)


def factor_block(ab, t_ref, v_ref):
    last = NB // TILE - 1

    def step(t, _):
        rows = pl.ds(pl.multiple_of(t * TILE, TILE), TILE)
        t_ref[...] = ab[rows, rows]
        tile_factor(t_ref, v_ref)
        ab[rows, rows] = t_ref[...]
        ab[rows, pl.ds(pl.multiple_of(NB + t * TILE, TILE), TILE)] = v_ref[...]
        for tt in range(last + 1):
            here = slice(tt * TILE, tt * TILE + TILE)
            below = slice(tt * TILE + TILE, NB)

            @pl.when(t == tt)
            def _():
                v = v_ref[...]
                if tt:
                    w = mm(v, ab[here, NB : NB + tt * TILE], 1, 0)
                    ab[here, NB : NB + tt * TILE] = w
                if tt < last:
                    u = mm(v, ab[here, below], 1, 0)
                    ab[here, below] = u
                    ab[below, below] = ab[below, below] - mm(u, u, 0, 0)
                    inv = slice(NB, NB + tt * TILE + TILE)
                    ab[below, inv] = ab[below, inv] - mm(u, ab[here, inv], 0, 0)
        return 0

    lax.fori_loop(0, last + 1, step, 0)


def eye_into(ref):
    r = lax.broadcasted_iota(jnp.int32, (NB, NB), 0)
    c = lax.broadcasted_iota(jnp.int32, (NB, NB), 1)
    ref[...] = jnp.where(r == c, 1.0, 0.0).astype(jnp.float32)


def factor_kernel(g, both_ab, y_ref, t_ref, v_ref):
    def panel(p, carry):
        ab = both_ab.at[p]
        eye_into(ab.at[:, NB : 2 * NB])

        @pl.when(p == 0)
        def _():
            ab[:, 0:NB] = g[0]

        @pl.when(p == 1)
        def _():
            for q in range(4):
                here = slice(q * TILE, q * TILE + TILE)
                y_ref[here, :] = mm(both_ab[0, here, NB : NB + q * TILE + TILE], g[1, :, 0 : q * TILE + TILE], 1, 1)
            for q in range(4):
                here, right = slice(q * TILE, q * TILE + TILE), slice(q * TILE, NB)
                ab[here, right] = g[2, here, right] - mm(y_ref[:, here], y_ref[:, right], 0, 0)

        factor_block(ab, t_ref, v_ref)
        return carry

    lax.fori_loop(0, 2, panel, 0)


def factors(g):
    f = jnp.float32
    vm = pl.BlockSpec(memory_space=pltpu.VMEM)
    return pl.pallas_call(
        factor_kernel,
        out_shape=[jax.ShapeDtypeStruct((2, NB, 2 * NB), f), jax.ShapeDtypeStruct((NB, NB), f)],
        in_specs=[vm], out_specs=[vm] * 2,
        scratch_shapes=[pltpu.VMEM((TILE, TILE), f), pltpu.VMEM((TILE, TILE), f)],
        compiler_params=pltpu.CompilerParams(vmem_limit_bytes=14 * 2**20),
        name="factors",
    )(g)


def split(v):
    hi = v.astype(jnp.bfloat16)
    return hi, (v - hi.astype(jnp.float32)).astype(jnp.bfloat16)


def dot3(a, b, ca, cb):
    dims = (((ca,), (cb,)), ((), ()))
    f = lambda p, q: lax.dot_general(p, q, dims, preferred_element_type=jnp.float32)
    return f(a[1], b[0]) + f(a[0], b[1]) + f(a[0], b[0])


HR = 256


def tri3(a, low, ca):
    h = NB // 2
    if ca == 1:
        first = dot3([v[:, :h] for v in a], [v[:h, :h] for v in low], 1, 1)
        return jnp.concatenate([first, dot3(a, [v[h:, :] for v in low], 1, 1)], axis=1)
    first = dot3([v[:h, :h] for v in low], [v[:h, :] for v in a], 1, 0)
    return jnp.concatenate([first, dot3([v[h:, :] for v in low], a, 1, 0)], axis=0)


def update_kernel(pos, m, rp, cp, ab, y, out, wh, wl, l1h, l1l, l2h, l2l, yh, yl, low, lh, ll):
    g = pl.program_id(0)
    k, r, c = pos[0], pos[1], pos[2]

    @pl.when(g == 0)
    def _():
        l1h[...], l1l[...] = split(ab[0, :, NB : 2 * NB])
        l2h[...], l2l[...] = split(ab[1, :, NB : 2 * NB])
        yh[...], yl[...] = split(y[...])
        tri = lax.broadcasted_iota(jnp.int32, (NB, NB), 0) <= lax.broadcasted_iota(jnp.int32, (NB, NB), 1)
        def lower(p):
            @pl.when(c == lax.rem(k + p, 16))
            def _():
                low[p] = jnp.where(tri, ab[p, :, 0:NB], 0.0).T

        loop(2, lower)

        def columns(q):
            j, h = q // 2, lax.rem(q, 2)

            @pl.when(16 * j + c > k)
            def _():
                    cols = pl.ds(pl.multiple_of(q * 256, 256), 256)
                    a = [jnp.concatenate([cp[p, pl.ds(4 * h + 2 * t + j, NB, stride=8), :] for t in (0, 1)], axis=1) for p in range(2)]
                    ws = split(tri3(split(a[0]), (l1h[...], l1l[...]), 0))
                    s = a[1] - dot3((yh[...], yl[...]), ws, 0, 0)
                    w2 = jnp.where(16 * j + c > k + 1, tri3(split(s), (l2h[...], l2l[...]), 0), 0.0)
                    wh[0:NB, cols], wl[0:NB, cols] = ws
                    wh[NB : 2 * NB, cols], wl[NB : 2 * NB, cols] = split(w2)

        loop(4, columns)

    i, half = g // 2, lax.rem(g, 2)
    row = 8 * i + r

    @pl.when(row <= k)
    def _():
        out[...] = m[...]

    @pl.when(row > k)
    def _():
        xa = tri3(split(rp[0, 0]), (l1h[...], l1l[...]), 1)
        xs = split(xa)
        s = rp[1, 0] - dot3(xs, (yh[...], yl[...]), 1, 0)
        x2 = jnp.where(row > k + 1, tri3(split(s), (l2h[...], l2l[...]), 1), 0.0)
        x2s = split(x2)
        lh[:, 0:NB], ll[:, 0:NB] = xs
        lh[:, NB : 2 * NB], ll[:, NB : 2 * NB] = x2s

        def columns(q):
            j, h = q // 2, lax.rem(q, 2)

            @pl.when(16 * j + c <= k)
            def _():
                for t in range(2):
                    rows = pl.ds(4 * h + 2 * t + j, HR, stride=8)
                    out[rows, :] = m[rows, :]

            @pl.when(16 * j + c > k)
            def _():
                cols = pl.ds(pl.multiple_of(q * 256, 256), 256)
                prod = dot3((lh[...], ll[...]), (wh[:, cols], wl[:, cols]), 1, 0)
                for t in range(2):
                    rows = pl.ds(4 * h + 2 * t + j, HR, stride=8)
                    out[rows, :] = m[rows, :] - prod[:, t * 128 : t * 128 + 128]

        loop(4, columns)

        for x, kk in ((xa, k), (x2, k + 1)):
            @pl.when(jnp.logical_and(c == lax.rem(kk, 16), row > kk))
            def _():
                for t in range(4):
                    out[pl.ds(2 * t + kk // 16, HR, stride=8), :] = x[:, t * 128 : t * 128 + 128]

    for p in range(2):
        kk = k + p

        @pl.when(jnp.logical_and(c == lax.rem(kk, 16), row == kk))
        def _():
            for t in range(4):
                out[pl.ds(2 * t + kk // 16, HR, stride=8), :] = low[p, pl.ds(pl.multiple_of(half * HR, HR), HR), t * 128 : t * 128 + 128]


def update(pos, m, rp, cp, ab, y):
    full = lambda *s: pl.BlockSpec(s, lambda g: (0,) * len(s))
    b = jnp.bfloat16
    return pl.pallas_call(
        update_kernel,
        grid=(8,),
        out_shape=jax.ShapeDtypeStruct((16384, 128), jnp.float32),
        in_specs=[
            pl.BlockSpec(memory_space=pltpu.SMEM),
            pl.BlockSpec((8 * HR, 128), lambda g: (g, 0)),
            pl.BlockSpec((2, 1, HR, NB), lambda g: (0, g // 2, g % 2, 0)),
            full(2, 4096, 128), full(2, NB, 2 * NB), full(NB, NB),
        ],
        out_specs=pl.BlockSpec((8 * HR, 128), lambda g: (g, 0)),
        scratch_shapes=[pltpu.VMEM((2 * NB, 2 * NB), b), pltpu.VMEM((2 * NB, 2 * NB), b)] + [pltpu.VMEM((NB, NB), b)] * 6 + [pltpu.VMEM((2, NB, NB), jnp.float32), pltpu.VMEM((HR, 2 * NB), b), pltpu.VMEM((HR, 2 * NB), b)],
        compiler_params=pltpu.CompilerParams(vmem_limit_bytes=34 * 2**20),
        name="trailing",
    )(pos, m, rp, cp, ab, y)


def per_device(matrix_in, panel_start):
    k = panel_start[0]
    flat = matrix_in.reshape(4, NB, 2, 4, 128).transpose(0, 1, 3, 2, 4).reshape(16384, 128)
    rp, cp, g = lax.switch(k, [functools.partial(gather, kk) for kk in range(30)], flat)
    ab, y = factors(g)
    pos = jnp.stack([k, lax.axis_index("row"), lax.axis_index("col")]).astype(jnp.int32)
    out = update(pos, flat, rp, cp, ab, y)
    return out.reshape(4, NB, 4, 2, 128).transpose(0, 1, 3, 2, 4).reshape(4, NB, 2, NB)


def solution(mesh):
    return jax.shard_map(
        per_device,
        mesh=mesh,
        in_specs=(P(None, "row", None, "col"), P()),
        out_specs=P(None, "row", None, "col"),
        check_vma=False,
    )
```
